32 devices in a mesh: dp: 16 (over z, y, core), mp: 2 (over x).
Axes of the slice: x: 2, y: 2, z: 4, core: 2. Of those that a mesh axis runs over, the one named last changes fastest.
Arguments:
- features: bfloat16 [768, 384], P('dp'), may hold values from -100 to 100
- teacher_weight: float32 [384, 131072], P(None, ('dp', 'mp')), may hold values from -250 to 250
- student_weight: float32 [384, 131072], P(None, ('dp', 'mp')), may hold values from -24 to 24
- center: float32 [131072], P(('dp', 'mp')), may hold values from -1 to 1
Outputs:
- blended: float32 [384, 131072], P(None, ('dp', 'mp'))
- new_center: float32 [131072], P(('dp', 'mp'))
- log_targets: float32 [768, 131072], P(None, ('dp', 'mp'))
The draws below stay inside these ranges and needn't reach their ends.
All inputs are finite; a program needn't handle non-finite values.
Results may differ from the reference program's by a relative error of at most 0.0003.
Values may be sent and summed in bfloat16 or wider, within the bound.
A program may use at most 64 MiB of HBM per device.

```python
import math
import jax
import jax.numpy as jnp
from jax import lax

D = 384
K = 131072
IMAGES = 768


def mean_direction(key):
    return jax.random.normal(jax.random.fold_in(key, 101), (D,), jnp.float32)


def draw_features(key, part):
    shared = mean_direction(key)
    jitter_key, scale_key = jax.random.split(jax.random.fold_in(key, 202))
    jitter = jax.random.normal(jitter_key, (IMAGES, D), jnp.float32)
    scales = jnp.exp(jax.random.uniform(scale_key, (IMAGES, 1), jnp.float32) * math.log(10.0))
    return jnp.clip((shared[None, :] + jitter) * scales, -100.0, 100.0).astype(jnp.bfloat16)


def draw_teacher_weight(key, part):
    shared = mean_direction(key)
    jitter_key, align_key, scale_key = jax.random.split(jax.random.fold_in(key, 303), 3)
    jitter = jax.random.normal(jitter_key, (D, K), jnp.float32)
    alignment = 0.6 * jax.random.normal(align_key, (1, K), jnp.float32)
    scales = jnp.exp(jax.random.uniform(scale_key, (1, K), jnp.float32) * math.log(10.0))
    return jnp.clip(scales * (alignment * shared[:, None] + jitter), -250.0, 250.0)


def draw_center(key, part):
    trend = 0.08 * (1.0 - 2.0 * jnp.arange(K, dtype=jnp.float32) / K)
    value_key = jax.random.fold_in(key, 404)
    spread = 0.4 * jax.random.uniform(value_key, (K,), jnp.float32, -1.0, 1.0)
    return trend + spread


def block_levels(rng, dims, shards, smallest, high):
    level = 1.0
    for dim, shards_of in shards:
        heights = jax.random.uniform(jax.random.fold_in(jax.random.fold_in(rng, 6), dim), (shards_of,), jnp.float32, smallest / len(shards), high / len(shards))
        level = level * jnp.repeat(jnp.exp(heights), dims[dim] // shards_of).reshape((-1,) + (1,) * (len(dims) - 1 - dim))
    return level


def centred(rng, shape, width, reach, cuts=(), kind=jnp.bfloat16):
    drawn = width * jax.random.normal(rng, shape, jnp.float32)
    if cuts:
        drawn = drawn * block_levels(rng, shape, cuts, -0.22, 0.18)
    return jnp.clip(drawn, -reach, reach).astype(kind)


def setup_inputs(seed: int = 0) -> dict:
    keys = jax.random.split(jax.random.key(seed), 5)
    features = draw_features(jax.random.fold_in(keys[4], 71), 0)
    teacher_weight = draw_teacher_weight(jax.random.fold_in(keys[4], 71), 0)
    student_weight = centred(keys[2], (D, K), 4.0, 24.0, ((1, 32),), jnp.float32)
    center = draw_center(jax.random.fold_in(keys[4], 71), 0)
    return {"features": features, "teacher_weight": teacher_weight, "student_weight": student_weight, "center": center}


ema_momentum = 0.994
center_momentum = 0.9
teacher_temp = 0.07
epsilon = 1e-06

def reference(features, teacher_weight, student_weight, center):
    blended = ema_momentum * teacher_weight + (1.0 - ema_momentum) * student_weight
    col_norm = jnp.sqrt(lax.optimization_barrier(jnp.sum(blended * blended, axis=0, keepdims=True)) + epsilon)
    protos = (blended / col_norm).astype(jnp.bfloat16)
    wide_feats = features.astype(jnp.float32)
    row_norm = jnp.sqrt(lax.optimization_barrier(jnp.sum(wide_feats * wide_feats, axis=1, keepdims=True)) + epsilon)
    unit_rows = (wide_feats / row_norm).astype(jnp.bfloat16)
    logits = jnp.dot(unit_rows, protos, preferred_element_type=jnp.float32)
    column_sums = lax.optimization_barrier(jnp.sum(logits, axis=0))
    new_center = center_momentum * center + (1.0 - center_momentum) * (column_sums / IMAGES)
    shifted = (logits - new_center[None, :]) / teacher_temp
    totals = lax.optimization_barrier(jnp.sum(jnp.exp(shifted), axis=1))
    log_targets = shifted - jnp.log(totals)[:, None]
    return (blended, new_center, log_targets)
```

```python
import functools

import jax
import jax.numpy as jnp
from jax import lax
from jax.experimental import pallas as pl
from jax.experimental.pallas import tpu as pltpu
from jax.sharding import PartitionSpec as P

ema_momentum = 0.994
center_momentum = 0.9
teacher_temp = 0.07
epsilon = 1e-06

MESH = pl.DeviceIdType.MESH
LANES = 128


def targets_kernel(
    n_dp, n_mp, blend_cols, dot_cols,
    feats_ref, teacher_ref, student_ref, center_ref,
    blended_ref, shifted_ref, new_center_ref, logs_ref,
    raw, student, protos, rows_ref, part, mine, others, old_center,
    own_sem, center_sem, teacher_sem, student_sem,
    send_sem, recv_sem, pass_sem, passed_sem, total_send, total_recv,
):
    dp, mp = lax.axis_index("dp"), lax.axis_index("mp")
    me = dp * n_mp + mp
    n = n_dp * n_mp
    per = raw.shape[1]
    depth, cols = blended_ref.shape
    images = shifted_ref.shape[0]
    extra = rows_ref.shape[0] - images

    blends = cols // blend_cols
    loads = []
    for j in range(blends):
        at = pl.ds(j * blend_cols, blend_cols)
        pair = (
            pltpu.make_async_copy(teacher_ref.at[:, at], blended_ref.at[:, at], teacher_sem.at[j]),
            pltpu.make_async_copy(student_ref.at[:, at], student.at[:, at], student_sem.at[j]),
        )
        for copy in pair:
            copy.start()
        loads.append(pair)
    own = pltpu.make_async_copy(feats_ref, raw.at[dp], own_sem)
    own.start()
    centers_in = pltpu.make_async_copy(center_ref, old_center, center_sem)
    centers_in.start()

    barrier = pltpu.get_barrier_semaphore()

    def greet(o, _):
        peer = lax.rem(me + o, n)
        pl.semaphore_signal(barrier, inc=1, device_id=(peer // n_mp, lax.rem(peer, n_mp)), device_id_type=MESH)
        return 0

    lax.fori_loop(1, n, greet, 0)

    def blend(j):
        for copy in loads[j]:
            copy.wait()
        for c in range(j * blend_cols, (j + 1) * blend_cols, LANES):
            at = slice(c, c + LANES)
            mixed = ema_momentum * blended_ref[:, at] + (1.0 - ema_momentum) * student[:, at]
            blended_ref[:, at] = mixed
            squares = jnp.sum(mixed * mixed, axis=0, keepdims=True)
            protos[:, at] = (mixed * (1.0 / jnp.sqrt(squares + epsilon))).astype(jnp.bfloat16)

    early = min(blends, max(1, blends // 2))
    for j in range(early):
        blend(j)

    pl.semaphore_wait(barrier, n - 1)
    chips = n_dp // 2
    chip, core = dp // 2, lax.rem(dp, 2)
    mate = 2 * chip + 1 - core

    def to_chip(o):
        return pltpu.make_async_remote_copy(
            src_ref=feats_ref,
            dst_ref=raw.at[dp],
            send_sem=send_sem.at[o],
            recv_sem=recv_sem.at[o],
            device_id=(2 * lax.rem(chip + o, chips) + core, mp),
            device_id_type=MESH,
        )

    def source(o):
        return 2 * lax.rem(chip + chips - o, chips) + core

    def to_mate(o):
        src = source(o)
        return pltpu.make_async_remote_copy(
            src_ref=raw.at[src],
            dst_ref=raw.at[src],
            send_sem=pass_sem.at[o],
            recv_sem=passed_sem.at[o],
            device_id=(mate, mp),
            device_id_type=MESH,
        )

    def send(o, _):
        to_chip(o).start()
        return 0

    lax.fori_loop(1, chips, send, 0)

    for j in range(early, blends):
        blend(j)

    def unit(piece, total):
        wide = raw[piece].astype(jnp.float32)
        norm = jnp.sqrt(jnp.sum(wide * wide, axis=1, keepdims=True) + epsilon)
        rows = (wide / norm).astype(jnp.bfloat16)
        rows_ref[pl.ds(pl.multiple_of(extra + piece * per, 16), per), :] = rows
        return total + jnp.sum(rows.astype(jnp.float32), axis=0, keepdims=True)

    own.wait()
    centers_in.wait()
    to_mate(0).start()
    total = unit(dp, jnp.zeros((1, depth), jnp.float32))

    def relay(o, total):
        to_chip(o).wait_recv()
        to_mate(o).start()
        return unit(source(o), total)

    total = lax.fori_loop(1, chips, relay, total)

    def passed(o, total):
        to_mate(o).wait_recv()
        return unit(source(o) + 1 - 2 * core, total)

    total = lax.fori_loop(0, chips, passed, total)

    high = total.astype(jnp.bfloat16).astype(jnp.float32)
    middle = (total - high).astype(jnp.bfloat16).astype(jnp.float32)
    low = total - high - middle
    row = lax.broadcasted_iota(jnp.int32, (extra, depth), 0)
    pieces = jnp.where(row == 0, high, jnp.where(row == 1, middle, jnp.where(row == 2, low, 0.0)))
    rows_ref[0:extra, :] = pieces.astype(jnp.bfloat16)

    part[...] = jnp.zeros_like(part)
    block = 64

    def targets(j, _):
        start = pl.multiple_of(j * dot_cols, dot_cols)
        logits = jnp.dot(rows_ref[...], protos[:, pl.ds(start, dot_cols)], preferred_element_type=jnp.float32)
        centers = []
        for t in range(dot_cols // LANES):
            sums = jnp.sum(logits[0:8, t * LANES:(t + 1) * LANES], axis=0, keepdims=True)
            spot = pl.ds(j * (dot_cols // LANES) + t, 1)
            fresh = center_momentum * old_center[spot, :] + (1.0 - center_momentum) * (sums / images)
            new_center_ref[spot, :] = fresh
            centers.append(fresh)
        for r in range(0, images, block):
            acc = part[r:r + block, :]
            for t, fresh in enumerate(centers):
                logit = logits[extra + r:extra + r + block, t * LANES:(t + 1) * LANES]
                shifted = (logit - fresh) * (1.0 / teacher_temp)
                shifted_ref[r:r + block, pl.ds(pl.multiple_of(start + t * LANES, LANES), LANES)] = shifted
                acc = acc + jnp.exp(shifted)
            part[r:r + block, :] = acc
        return 0

    lax.fori_loop(0, cols // dot_cols, targets, 0, unroll=2 if cols // dot_cols % 2 == 0 else 1)

    mine[...] = jnp.ones_like(mine)
    for i in range(images // LANES):
        mine[i:i + 1, :] = jnp.sum(part[i * LANES:(i + 1) * LANES, :].T, axis=0, keepdims=True)

    def share(o, _):
        peer = lax.rem(me + o, n)
        pltpu.make_async_remote_copy(
            src_ref=mine,
            dst_ref=others.at[o - 1],
            send_sem=total_send,
            recv_sem=total_recv,
            device_id=(peer // n_mp, lax.rem(peer, n_mp)),
            device_id_type=MESH,
        ).start()
        return 0

    lax.fori_loop(1, n, share, 0)

    def sent(o, _):
        to_chip(o).wait_send()
        return 0

    lax.fori_loop(1, chips, sent, 0)

    def handed(o, _):
        to_mate(o).wait_send()
        return 0

    lax.fori_loop(0, chips, handed, 0)

    pltpu.make_async_copy(others, others, total_recv).wait()
    logs = jnp.log(mine[...] + jnp.sum(others[...], axis=0))
    for i in range(images // LANES):
        logs_ref[i * LANES:(i + 1) * LANES, :] = jnp.broadcast_to(logs[i:i + 1, :], (LANES, LANES)).T
    pltpu.make_async_copy(others, others, total_send).wait()


def finish_kernel(
    chunks, blended_in, shifted_ref, center_in, logs_ref,
    blended_out, center_out, out_ref, stage, blended_sem, center_sem, out_sem,
):
    images, cols = shifted_ref.shape
    step = images // chunks
    center = pltpu.make_async_copy(center_in, center_out, center_sem)
    blended = pltpu.make_async_copy(blended_in, blended_out, blended_sem)
    waits = [center, blended]
    center.start()
    blended.start()
    for i in range(chunks):
        log = logs_ref[i * step:(i + 1) * step, :]
        for c in range(0, cols, LANES):
            stage[i * step:(i + 1) * step, c:c + LANES] = shifted_ref[i * step:(i + 1) * step, c:c + LANES] - log
        at = pl.ds(i * step, step)
        copy = pltpu.make_async_copy(stage.at[at, :], out_ref.at[at, :], out_sem.at[i])
        copy.start()
        waits.append(copy)
    for copy in waits:
        copy.wait()


def solution(mesh):
    n_dp, n_mp = mesh.shape["dp"], mesh.shape["mp"]
    n = n_dp * n_mp

    def shards(features, teacher_weight, student_weight, center):
        per, depth = features.shape
        cols = teacher_weight.shape[1]
        images = per * n_dp
        tiles = cols // LANES
        blend_cols = min(cols, 512)
        dot_cols = min(cols, 512)
        held = -(-images // (8 * LANES)) * 8
        f32 = jnp.float32
        whole = pl.BlockSpec(memory_space=pltpu.VMEM)
        far = pl.BlockSpec(memory_space=pl.ANY)
        near = pl.BlockSpec(memory_space=pltpu.HBM)
        dma = pltpu.SemaphoreType.DMA
        blended, shifted, new_center, logs = pl.pallas_call(
            functools.partial(targets_kernel, n_dp, n_mp, blend_cols, dot_cols),
            out_shape=(
                pltpu.VMEM((depth, cols), f32),
                pltpu.VMEM((images, cols), f32),
                pltpu.VMEM((tiles, LANES), f32),
                pltpu.VMEM((images, LANES), f32),
            ),
            in_specs=[near] * 4,
            out_specs=(whole, whole, whole, whole),
            scratch_shapes=[
                pltpu.VMEM((n_dp, per, depth), jnp.bfloat16),
                pltpu.VMEM((depth, cols), f32),
                pltpu.VMEM((depth, cols), jnp.bfloat16),
                pltpu.VMEM((16 + images, depth), jnp.bfloat16),
                pltpu.VMEM((images, LANES), f32),
                pltpu.VMEM((held, LANES), f32),
                pltpu.VMEM((n - 1, held, LANES), f32),
                pltpu.VMEM((tiles, LANES), f32),
                dma, dma, dma((cols // blend_cols,)), dma((cols // blend_cols,)),
                dma((n_dp // 2,)), dma((n_dp // 2,)), dma((n_dp // 2,)), dma((n_dp // 2,)),
                dma, dma,
            ],
            compiler_params=pltpu.CompilerParams(
                collective_id=0, has_side_effects=True, vmem_limit_bytes=20 * 2**20
            ),
            name="targets",
        )(features, teacher_weight, student_weight, center.reshape(tiles, LANES))
        chunks = 16
        blended, new_center, log_targets = pl.pallas_call(
            functools.partial(finish_kernel, chunks),
            out_shape=(
                jax.ShapeDtypeStruct((depth, cols), f32),
                jax.ShapeDtypeStruct((tiles, LANES), f32),
                jax.ShapeDtypeStruct((images, cols), f32),
            ),
            in_specs=[whole] * 4,
            out_specs=(far, far, far),
            scratch_shapes=[pltpu.VMEM((images, cols), f32), dma, dma, dma((chunks,))],
            compiler_params=pltpu.CompilerParams(vmem_limit_bytes=16 * 2**20),
            name="finish",
        )(blended, shifted, new_center, logs)
        return blended, new_center.reshape(cols), log_targets

    placed = (P("dp", None), P(None, ("dp", "mp")), P(None, ("dp", "mp")), P(("dp", "mp")))
    return jax.shard_map(
        shards,
        mesh=mesh,
        in_specs=placed,
        out_specs=(P(None, ("dp", "mp")), P(("dp", "mp")), P(None, ("dp", "mp"))),
        check_vma=False,
    )
```

```python
import functools

import jax
import jax.numpy as jnp
from jax import lax
from jax.experimental import pallas as pl
from jax.experimental.pallas import tpu as pltpu
from jax.sharding import PartitionSpec as P

ema_momentum = 0.994
center_momentum = 0.9
teacher_temp = 0.07
epsilon = 1e-06

MESH = pl.DeviceIdType.MESH
LANES = 128


def targets_kernel(
    n_dp, n_mp, blend_cols, dot_cols,
    feats_ref, teacher_ref, student_ref, center_ref,
    blended_ref, shifted_ref, new_center_ref, logs_ref,
    raw, student, protos, rows_ref, part, mine, others, old_center,
    own_sem, center_sem, teacher_sem, student_sem,
    send_sem, recv_sem, pass_sem, passed_sem, total_send, total_recv,
):
    dp, mp = lax.axis_index("dp"), lax.axis_index("mp")
    n = n_dp * n_mp
    per = raw.shape[2]
    depth, cols = blended_ref.shape
    images = shifted_ref.shape[0]
    extra = rows_ref.shape[0] - images

    blends = cols // blend_cols
    loads = []
    for j in range(blends):
        at = pl.ds(j * blend_cols, blend_cols)
        pair = (
            pltpu.make_async_copy(teacher_ref.at[:, at], blended_ref.at[:, at], teacher_sem.at[j]),
            pltpu.make_async_copy(student_ref.at[:, at], student.at[:, at], student_sem.at[j]),
        )
        for copy in pair:
            copy.start()
        loads.append(pair)
    own = pltpu.make_async_copy(feats_ref, raw.at[lax.rem(dp, 2), dp // 2], own_sem)
    own.start()
    centers_in = pltpu.make_async_copy(center_ref, old_center, center_sem)
    centers_in.start()

    barrier = pltpu.get_barrier_semaphore()

    rings = n_dp // 4
    outer, inner, core = dp // 4, lax.rem(dp // 2, 2), lax.rem(dp, 2)
    mate = dp + 1 - 2 * core
    beside = dp + 2 - 4 * inner

    def each_peer(act):
        for b in range(1, n_mp):
            act(b - 1, dp, lax.rem(mp + b, n_mp))

        def row(a, _):
            there = lax.rem(dp + a, n_dp)
            for b in range(n_mp):
                act(a * n_mp + b - 1, there, lax.rem(mp + b, n_mp))
            return 0

        lax.fori_loop(1, n_dp, row, 0, unroll=n_dp <= 16)

    each_peer(lambda slot, d, m: pl.semaphore_signal(barrier, inc=1, device_id=(d, m), device_id_type=MESH))

    def place(o, f):
        near = inner + f * (1 - 2 * inner)
        return 2 * lax.rem(outer + rings - o, rings) + near

    def around(o):
        return pltpu.make_async_remote_copy(
            src_ref=feats_ref,
            dst_ref=raw.at[core, dp // 2],
            send_sem=send_sem.at[o],
            recv_sem=recv_sem.at[o],
            device_id=(4 * lax.rem(outer + o, rings) + 2 * inner + core, mp),
            device_id_type=MESH,
        )

    def across(o):
        spot = raw.at[core, place(o, 0)]
        return pltpu.make_async_remote_copy(
            src_ref=feats_ref if o == 0 else spot,
            dst_ref=spot,
            send_sem=send_sem.at[rings + o],
            recv_sem=recv_sem.at[rings + o],
            device_id=(beside, mp),
            device_id_type=MESH,
        )

    def to_mate(o, f):
        spot = raw.at[core, place(o, f)]
        return pltpu.make_async_remote_copy(
            src_ref=feats_ref if o == 0 and f == 0 else spot,
            dst_ref=spot,
            send_sem=pass_sem.at[f * rings + o],
            recv_sem=passed_sem.at[f * rings + o],
            device_id=(mate, mp),
            device_id_type=MESH,
        )

    pl.semaphore_wait(barrier, n - 1)
    for o in sorted(range(1, rings), key=lambda o: -min(o, rings - o)):
        around(o).start()
    across(0).start()
    to_mate(0, 0).start()

    def blend(j):
        for copy in loads[j]:
            copy.wait()
        for c in range(j * blend_cols, (j + 1) * blend_cols, LANES):
            at = slice(c, c + LANES)
            mixed = ema_momentum * blended_ref[:, at] + (1.0 - ema_momentum) * student[:, at]
            blended_ref[:, at] = mixed
            squares = jnp.sum(mixed * mixed, axis=0, keepdims=True)
            protos[:, at] = (mixed * (1.0 / jnp.sqrt(squares + epsilon))).astype(jnp.bfloat16)

    for j in range(blends):
        blend(j)

    def unit(half):
        wide = raw[half].astype(jnp.float32)
        norm = jnp.sqrt(jnp.sum(wide * wide, axis=2, keepdims=True) + epsilon)
        rows = (wide / norm).astype(jnp.bfloat16)
        for c in range(n_dp // 2):
            rows_ref[pl.ds(pl.multiple_of(extra + (2 * c + half) * per, 16), per), :] = rows[c]
        return jnp.sum(jnp.sum(rows.astype(jnp.float32), axis=0), axis=0, keepdims=True)

    own.wait()
    centers_in.wait()
    for o in sorted(range(1, rings), key=lambda o: min(o, rings - o)):
        around(o).wait_recv()
        across(o).start()
        to_mate(o, 0).start()
    for o in sorted(range(rings), key=lambda o: min(o, rings - o)):
        across(o).wait_recv()
        to_mate(o, 1).start()
    total = unit(core)
    for f in range(2):
        for o in range(rings):
            to_mate(o, f).wait_recv()
    total = total + unit(1 - core)

    high = total.astype(jnp.bfloat16).astype(jnp.float32)
    middle = (total - high).astype(jnp.bfloat16).astype(jnp.float32)
    low = total - high - middle
    row = lax.broadcasted_iota(jnp.int32, (extra, depth), 0)
    pieces = jnp.where(row == 0, high, jnp.where(row == 1, middle, jnp.where(row == 2, low, 0.0)))
    rows_ref[0:extra, :] = pieces.astype(jnp.bfloat16)

    part[...] = jnp.zeros_like(part)
    block = 64

    def targets(j, _):
        start = pl.multiple_of(j * dot_cols, dot_cols)
        logits = jnp.dot(rows_ref[...], protos[:, pl.ds(start, dot_cols)], preferred_element_type=jnp.float32)
        centers = []
        for t in range(dot_cols // LANES):
            sums = jnp.sum(logits[0:8, t * LANES:(t + 1) * LANES], axis=0, keepdims=True)
            spot = pl.ds(j * (dot_cols // LANES) + t, 1)
            fresh = center_momentum * old_center[spot, :] + (1.0 - center_momentum) * (sums / images)
            new_center_ref[spot, :] = fresh
            centers.append(fresh)
        for r in range(0, images, block):
            acc = part[r:r + block, :]
            for t, fresh in enumerate(centers):
                logit = logits[extra + r:extra + r + block, t * LANES:(t + 1) * LANES]
                shifted = (logit - fresh) * (1.0 / teacher_temp)
                shifted_ref[r:r + block, pl.ds(pl.multiple_of(start + t * LANES, LANES), LANES)] = shifted
                acc = acc + jnp.exp(shifted)
            part[r:r + block, :] = acc
        return 0

    lax.fori_loop(0, cols // dot_cols, targets, 0, unroll=2 if cols // dot_cols % 2 == 0 else 1)

    mine[...] = jnp.ones_like(mine)
    for i in range(images // LANES):
        mine[i:i + 1, :] = jnp.sum(part[i * LANES:(i + 1) * LANES, :].T, axis=0, keepdims=True)

    def share(slot, d, m):
        pltpu.make_async_remote_copy(
            src_ref=mine,
            dst_ref=others.at[slot],
            send_sem=total_send,
            recv_sem=total_recv,
            device_id=(d, m),
            device_id_type=MESH,
        ).start()

    each_peer(share)

    for o in range(rings):
        if o:
            around(o).wait_send()
        across(o).wait_send()
        for f in range(2):
            to_mate(o, f).wait_send()

    pltpu.make_async_copy(others, others, total_recv).wait()
    logs = jnp.log(mine[...] + jnp.sum(others[...], axis=0))
    for i in range(images // LANES):
        logs_ref[i * LANES:(i + 1) * LANES, :] = jnp.broadcast_to(logs[i:i + 1, :], (LANES, LANES)).T
    pltpu.make_async_copy(others, others, total_send).wait()


def finish_kernel(
    chunks, blended_in, shifted_ref, center_in, logs_ref,
    blended_out, center_out, out_ref, stage, blended_sem, center_sem, out_sem,
):
    images, cols = shifted_ref.shape
    step = images // chunks
    center = pltpu.make_async_copy(center_in, center_out, center_sem)
    blended = pltpu.make_async_copy(blended_in, blended_out, blended_sem)
    waits = [center, blended]
    center.start()
    blended.start()
    for i in range(chunks):
        log = logs_ref[i * step:(i + 1) * step, :]
        for c in range(0, cols, LANES):
            stage[i * step:(i + 1) * step, c:c + LANES] = shifted_ref[i * step:(i + 1) * step, c:c + LANES] - log
        at = pl.ds(i * step, step)
        copy = pltpu.make_async_copy(stage.at[at, :], out_ref.at[at, :], out_sem.at[i])
        copy.start()
        waits.append(copy)
    for copy in waits:
        copy.wait()


def solution(mesh):
    n_dp, n_mp = mesh.shape["dp"], mesh.shape["mp"]
    n = n_dp * n_mp

    def shards(features, teacher_weight, student_weight, center):
        per, depth = features.shape
        cols = teacher_weight.shape[1]
        images = per * n_dp
        tiles = cols // LANES
        blend_cols = min(cols, 512)
        dot_cols = min(cols, 512)
        held = -(-images // (8 * LANES)) * 8
        f32 = jnp.float32
        whole = pl.BlockSpec(memory_space=pltpu.VMEM)
        operands = (features, teacher_weight, student_weight, center.reshape(tiles, LANES))
        far = pl.BlockSpec(memory_space=pl.ANY)
        near = pl.BlockSpec(memory_space=pltpu.HBM)
        dma = pltpu.SemaphoreType.DMA
        blended, shifted, new_center, logs = pl.pallas_call(
            functools.partial(targets_kernel, n_dp, n_mp, blend_cols, dot_cols),
            out_shape=(
                pltpu.VMEM((depth, cols), f32),
                pltpu.VMEM((images, cols), f32),
                pltpu.VMEM((tiles, LANES), f32),
                pltpu.VMEM((images, LANES), f32),
            ),
            in_specs=[near] * 4,
            out_specs=(whole, whole, whole, whole),
            scratch_shapes=[
                pltpu.VMEM((2, n_dp // 2, per, depth), jnp.bfloat16),
                pltpu.VMEM((depth, cols), f32),
                pltpu.VMEM((depth, cols), jnp.bfloat16),
                pltpu.VMEM((16 + images, depth), jnp.bfloat16),
                pltpu.VMEM((images, LANES), f32),
                pltpu.VMEM((held, LANES), f32),
                pltpu.VMEM((n - 1, held, LANES), f32),
                pltpu.VMEM((tiles, LANES), f32),
                dma, dma, dma((cols // blend_cols,)), dma((cols // blend_cols,)),
                dma((n_dp // 2,)), dma((n_dp // 2,)), dma((n_dp // 2,)), dma((n_dp // 2,)),
                dma, dma,
            ],
            compiler_params=pltpu.CompilerParams(
                collective_id=0, has_side_effects=True, vmem_limit_bytes=20 * 2**20
            ),
            name="targets",
        )(*(pltpu.with_memory_space_constraint(x, pltpu.HBM) for x in operands))
        chunks = 16
        blended, new_center, log_targets = pl.pallas_call(
            functools.partial(finish_kernel, chunks),
            out_shape=(
                jax.ShapeDtypeStruct((depth, cols), f32),
                jax.ShapeDtypeStruct((tiles, LANES), f32),
                jax.ShapeDtypeStruct((images, cols), f32),
            ),
            in_specs=[whole] * 4,
            out_specs=(far, far, far),
            scratch_shapes=[pltpu.VMEM((images, cols), f32), dma, dma, dma((chunks,))],
            compiler_params=pltpu.CompilerParams(vmem_limit_bytes=16 * 2**20),
            name="finish",
        )(blended, shifted, new_center, logs)
        return blended, new_center.reshape(cols), log_targets

    placed = (P("dp", None), P(None, ("dp", "mp")), P(None, ("dp", "mp")), P(("dp", "mp")))
    return jax.shard_map(
        shards,
        mesh=mesh,
        in_specs=placed,
        out_specs=(P(None, ("dp", "mp")), P(("dp", "mp")), P(None, ("dp", "mp"))),
        check_vma=False,
    )
```
